32 devices in a mesh: dp: 4 (over x, y), tp: 8 (over z, core).
Axes of the slice: x: 2, y: 2, z: 4, core: 2. Of those that a mesh axis runs over, the one named last changes fastest.
Arguments:
- x_tokens: bfloat16 [8192, 2304], P(('dp', 'tp')), parts along dimension 0
- dy_tokens: bfloat16 [8192, 2304], P(('dp', 'tp')), parts along dimension 0
- w_q: bfloat16 [2304, 8, 256], P(None, 'tp')
- w_k: bfloat16 [2304, 4, 256], replicated
- w_v: bfloat16 [2304, 4, 256], replicated
- w_o: bfloat16 [8, 256, 2304], P('tp')
- w_gate: bfloat16 [2304, 9216], P(None, 'tp')
- w_up: bfloat16 [2304, 9216], P(None, 'tp')
- w_down: bfloat16 [9216, 2304], P('tp')
Outputs:
- output 1: bfloat16 [8192, 2304], P(('dp', 'tp')), parts along dimension 0
- output 2: float32 [9216, 8, 256], P('dp', 'tp'), parts along dimension 0
- output 3: float32 [32, 1152, 256], P(('dp', 'tp')), parts along dimension 0
- output 4: float32 [32, 1152, 256], P(('dp', 'tp')), parts along dimension 0
- output 5: float32 [32, 256, 2304], P(('dp', 'tp')), parts along dimension 0
- output 6: float32 [9216, 9216], P('dp', 'tp'), parts along dimension 0
- output 7: float32 [9216, 9216], P('dp', 'tp'), parts along dimension 0
- output 8: float32 [36864, 2304], P(('dp', 'tp')), parts along dimension 0
There are 4 independent parts. The reference program is written for one: setup_inputs(seed, part) draws one part's arguments, and reference() takes and returns one part's arrays. A program takes and returns all parts, laid end to end along the dimension named above; an argument that names none is the same for every part.
All inputs are finite; a program needn't handle non-finite values.
Results may differ from the reference program's by a relative error of at most 0.0130949.
Values are sent between devices in bfloat16 or wider.
A program may use at most 1 GiB of HBM per device.

```python
import jax
import jax.numpy as jnp
from jax import lax

SEQ_LEN = 2048
D_MODEL = 2304
Q_HEADS = 8
KV_HEADS = 4
HEAD_DIM = 256
FF_DIM = 9216
TP_SIZE = 8


def setup_inputs(seed: int = 0, part: int = 0) -> dict:
    part_key = jax.random.fold_in(jax.random.key(seed), part)
    token_keys = jax.random.split(part_key, 2)
    weight_keys = jax.random.split(jax.random.key(seed + 1), 7)
    model_scale = D_MODEL ** -0.5
    x_tokens = jax.random.normal(token_keys[0], (SEQ_LEN, D_MODEL), jnp.float32).astype(jnp.bfloat16)
    dy_tokens = jax.random.normal(token_keys[1], (SEQ_LEN, D_MODEL), jnp.float32).astype(jnp.bfloat16)
    w_q = (jax.random.normal(weight_keys[0], (D_MODEL, Q_HEADS, HEAD_DIM), jnp.float32) * model_scale).astype(jnp.bfloat16)
    w_k = (jax.random.normal(weight_keys[1], (D_MODEL, KV_HEADS, HEAD_DIM), jnp.float32) * model_scale).astype(jnp.bfloat16)
    w_v = (jax.random.normal(weight_keys[2], (D_MODEL, KV_HEADS, HEAD_DIM), jnp.float32) * model_scale).astype(jnp.bfloat16)
    w_o = (jax.random.normal(weight_keys[3], (Q_HEADS, HEAD_DIM, D_MODEL), jnp.float32) * (Q_HEADS * HEAD_DIM) ** -0.5).astype(jnp.bfloat16)
    w_gate = (jax.random.normal(weight_keys[4], (D_MODEL, FF_DIM), jnp.float32) * model_scale).astype(jnp.bfloat16)
    w_up = (jax.random.normal(weight_keys[5], (D_MODEL, FF_DIM), jnp.float32) * model_scale).astype(jnp.bfloat16)
    w_down = (jax.random.normal(weight_keys[6], (FF_DIM, D_MODEL), jnp.float32) * FF_DIM ** -0.5).astype(jnp.bfloat16)
    return {"x_tokens": x_tokens, "dy_tokens": dy_tokens, "w_q": w_q, "w_k": w_k, "w_v": w_v, "w_o": w_o, "w_gate": w_gate, "w_up": w_up, "w_down": w_down}


def head_grads(operands):
    q_one, k_one, v_one, do_one = operands
    score_scale = HEAD_DIM ** -0.5
    positions = jnp.arange(SEQ_LEN)
    causal = positions[:, None] >= positions[None, :]
    scores = jnp.dot(q_one, k_one.T, preferred_element_type=jnp.float32) * score_scale
    scores = jnp.where(causal, scores, -jnp.inf)
    attn_prob = jax.nn.softmax(scores, axis=-1)
    prob_low = attn_prob.astype(jnp.bfloat16)
    out_one = jnp.dot(prob_low, v_one, preferred_element_type=jnp.float32).astype(jnp.bfloat16)
    d_prob = jnp.dot(do_one, v_one.T, preferred_element_type=jnp.float32)
    row_delta = jnp.sum(do_one.astype(jnp.float32) * out_one.astype(jnp.float32), axis=-1, keepdims=True)
    d_scores = (attn_prob * (d_prob - row_delta)).astype(jnp.bfloat16)
    dq_one = (jnp.dot(d_scores, k_one, preferred_element_type=jnp.float32) * score_scale).astype(jnp.bfloat16)
    dk_one = jnp.dot(d_scores.T, q_one, preferred_element_type=jnp.float32) * score_scale
    dv_one = jnp.dot(prob_low.T, do_one, preferred_element_type=jnp.float32)
    return out_one, dq_one, dk_one, dv_one


def reference(x_tokens, dy_tokens, w_q, w_k, w_v, w_o, w_gate, w_up, w_down):
    group_size = Q_HEADS // KV_HEADS
    replicas = TP_SIZE // KV_HEADS
    d_block = D_MODEL // replicas
    x_f32 = x_tokens.astype(jnp.float32)
    dy_f32 = dy_tokens.astype(jnp.float32)
    q_heads = jnp.einsum("td,dhe->hte", x_f32, w_q.astype(jnp.float32)).astype(jnp.bfloat16)
    k_heads = jnp.einsum("td,dge->gte", x_f32, w_k.astype(jnp.float32)).astype(jnp.bfloat16)
    v_heads = jnp.einsum("td,dge->gte", x_f32, w_v.astype(jnp.float32)).astype(jnp.bfloat16)
    do_heads = jnp.einsum("tc,hec->hte", dy_f32, w_o.astype(jnp.float32)).astype(jnp.bfloat16)
    k_rep = jnp.repeat(k_heads, group_size, axis=0)
    v_rep = jnp.repeat(v_heads, group_size, axis=0)
    out_heads, dq_heads, dk_heads, dv_heads = lax.map(head_grads, (q_heads, k_rep, v_rep, do_heads))
    dk_sum = dk_heads.reshape(KV_HEADS, group_size, SEQ_LEN, HEAD_DIM).sum(axis=1).astype(jnp.bfloat16).astype(jnp.float32)
    dv_sum = dv_heads.reshape(KV_HEADS, group_size, SEQ_LEN, HEAD_DIM).sum(axis=1).astype(jnp.bfloat16).astype(jnp.float32)
    dq_f32 = dq_heads.astype(jnp.float32)
    dw_o = jnp.einsum("hte,tc->hec", out_heads.astype(jnp.float32), dy_f32)
    dw_q = jnp.einsum("td,hte->dhe", x_f32, dq_f32)
    x_split = x_f32.reshape(SEQ_LEN, replicas, d_block)
    dw_k = jnp.einsum("trd,gte->grde", x_split, dk_sum).reshape(TP_SIZE, d_block, HEAD_DIM)
    dw_v = jnp.einsum("trd,gte->grde", x_split, dv_sum).reshape(TP_SIZE, d_block, HEAD_DIM)
    gate_pre = jnp.dot(x_tokens, w_gate, preferred_element_type=jnp.float32).astype(jnp.bfloat16).astype(jnp.float32)
    up_pre = jnp.dot(x_tokens, w_up, preferred_element_type=jnp.float32).astype(jnp.bfloat16).astype(jnp.float32)
    gate_sig = jax.nn.sigmoid(gate_pre)
    gate_act = gate_pre * gate_sig
    hidden = (gate_act * up_pre).astype(jnp.bfloat16)
    dw_down = jnp.dot(hidden.T, dy_tokens, preferred_element_type=jnp.float32)
    d_hidden = jnp.dot(dy_tokens, w_down.T, preferred_element_type=jnp.float32)
    d_gate = (d_hidden * up_pre * gate_sig * (1.0 + gate_pre * (1.0 - gate_sig))).astype(jnp.bfloat16)
    d_up = (d_hidden * gate_act).astype(jnp.bfloat16)
    dw_gate = jnp.dot(x_tokens.T, d_gate, preferred_element_type=jnp.float32)
    dw_up = jnp.dot(x_tokens.T, d_up, preferred_element_type=jnp.float32)
    dx_sum = (jnp.einsum("hte,dhe->td", dq_f32, w_q.astype(jnp.float32))
              + jnp.einsum("gte,dge->td", dk_sum, w_k.astype(jnp.float32))
              + jnp.einsum("gte,dge->td", dv_sum, w_v.astype(jnp.float32))
              + jnp.dot(d_gate, w_gate.T, preferred_element_type=jnp.float32)
              + jnp.dot(d_up, w_up.T, preferred_element_type=jnp.float32))
    return (dx_sum.astype(jnp.bfloat16), dw_q, dw_k, dw_v, dw_o, dw_gate, dw_up, dw_down)
```

```python
import functools
import jax
import jax.numpy as jnp
from jax import lax
from jax.experimental import pallas as pl
from jax.experimental.pallas import tpu as pltpu
from jax.sharding import PartitionSpec as P


f32, bf16 = jnp.float32, jnp.bfloat16
NT = (((1,), (1,)), ((), ()))
TN = (((0,), (0,)), ((), ()))
NN = (((1,), (0,)), ((), ()))


def dot(a, b, dims=NN):
    return lax.dot_general(a, b, dims, preferred_element_type=f32)


def pick(chip, values):
    out = jnp.int32(values[-1])
    for i in range(len(values) - 1):
        out = jnp.where(chip == i, jnp.int32(values[i]), out)
    return out


X_ORDER = ((0, 1, 2, 3), (1, 0, 2, 3), (2, 3, 1, 0), (3, 2, 1, 0))
DY_ORDER = ((0, 3, 2, 1), (1, 3, 2, 0), (2, 3, 1, 0), (3, 2, 1, 0))
CHIPS = 4


def layer_kernel(x_loc, dy_loc, wg_h, wu_h, wq_h, wk_h, wv_h, wd_h, wo_h,
                 xy, ho_o, grads_o, dx_o,
                 w_in, wd, wo, buf, acts, do_all, dk_acc, dv_acc,
                 hobuf, dxbuf, recv, send, wsem, lsem, osem):
    piece, d_model = x_loc.shape
    seq_len = CHIPS * 2 * piece
    chunk = 2 * piece
    half = piece // 2
    head_dim = wo.shape[0]
    ff = wd.shape[0]
    width_in = acts.shape[1]
    q_at, k_at, v_at = (slice(2 * ff + i * head_dim, 2 * ff + (i + 1) * head_dim) for i in range(3))
    scale = head_dim ** -0.5
    me = lax.axis_index("tp")
    chip, core = me // 2, me % 2
    partner = me + 1 - 2 * core
    own = (x_loc, dy_loc)

    barrier = pltpu.get_barrier_semaphore()
    for step in range(1, 2 * CHIPS):
        pl.semaphore_signal(barrier, inc=1, device_id={"tp": (me + step) % (2 * CHIPS)},
                            device_id_type=pl.DeviceIdType.MESH)
    weights = [pltpu.make_async_copy(src, dst, wsem.at[i]) for i, (src, dst) in enumerate(
        ((wg_h, w_in.at[:, 0:ff]), (wu_h, w_in.at[:, ff:2 * ff]), (wq_h, w_in.at[:, q_at]), (wk_h, w_in.at[:, k_at]),
         (wv_h, w_in.at[:, v_at]), (wd_h, wd), (wo_h, wo)))]
    for copy in weights:
        copy.start()
    pl.semaphore_wait(barrier, 2 * CHIPS - 1)

    def rows_of(array, block, part):
        return pl.ds(pl.multiple_of(array * seq_len + block * piece + part * half, half), half)

    def remote(array, block, part, way, own_source=None):
        target = (me + 2, me - 2, partner)[way]
        there = xy.at[rows_of(array, block, part)]
        source = there if own_source is None else own_source.at[pl.ds(part * half, half)]
        return pltpu.make_async_remote_copy(
            src_ref=source, dst_ref=there, send_sem=send.at[way, array, block // 2, part],
            recv_sem=recv.at[array, block, part], device_id={"tp": target}, device_id_type=pl.DeviceIdType.MESH)

    def send_own(array, way):
        for part in range(2):
            remote(array, me, part, way, own[array]).start()

    @pl.when(chip < CHIPS - 1)
    def _():
        send_own(0, 0)

    @pl.when(chip > 0)
    def _():
        send_own(0, 1)

    send_own(0, 2)
    send_own(1, 2)

    def event(k):
        j, part = k // 2, k % 2

        @pl.when((chip < CHIPS - 1) & (2 * chip == k))
        def _():
            send_own(1, 0)

        @pl.when((chip > 0) & (4 * (CHIPS - 1 - chip) == k))
        def _():
            send_own(1, 1)

        above = CHIPS - 1 - chip

        @pl.when(j < 2 * above)
        def _():
            array = jnp.where(j < above, 0, 1)
            block = 2 * jnp.where(j < above, chip + 1 + j, CHIPS - 1 - j + above) + core
            remote(array, block, part, 2).wait_recv()
            remote(array, block, part, 2).start()

            @pl.when(chip > 0)
            def _():
                remote(array, block, part, 1).start()

        below = chip

        @pl.when(j < 2 * below)
        def _():
            array = jnp.where(j < below, 0, 1)
            block = 2 * jnp.where(j < below, chip - 1 - j, chip - 1 - j + below) + core
            remote(array, block, part, 2).wait_recv()
            remote(array, block, part, 2).start()

            @pl.when(chip < CHIPS - 1)
            def _():
                remote(array, block, part, 0).start()

    def load(array, which):
        for part in range(2):
            remote(array, 2 * which + 1 - core, part, 2).wait_recv()
        copy = pltpu.make_async_copy(xy.at[pl.ds(pl.multiple_of(array * seq_len + which * chunk, chunk), chunk)],
                                     buf, lsem.at[0])
        copy.start()
        copy.wait()

    def rows_at(which):
        return pl.ds(pl.multiple_of(which * chunk, chunk), chunk)

    def look_up(orders, unit):
        return pick(unit, [pick(chip, [order[i] for order in orders]) for i in range(CHIPS)])

    keeps = [pltpu.make_async_copy(src, dxbuf.at[pl.ds(i * piece, piece)], lsem.at[i]) for i, src in enumerate(own)]
    for copy in keeps:
        copy.start()
    for copy in keeps:
        copy.wait()
    keeps = [pltpu.make_async_copy(dxbuf.at[pl.ds(i * piece, piece)],
                                   xy.at[pl.ds(pl.multiple_of(i * seq_len + me * piece, piece), piece)], lsem.at[i])
             for i in range(2)]
    for copy in keeps:
        copy.start()
    for copy in keeps:
        copy.wait()
    for copy in weights:
        copy.wait()

    def x_unit(unit, carry):
        @pl.when(unit > 0)
        def _():
            event(2 * unit - 2)
            event(2 * unit - 1)

        which = look_up(X_ORDER, unit)
        load(0, which)
        for cut in range(2):
            cols = slice(cut * width_in // 2, (cut + 1) * width_in // 2)
            acts[rows_at(which), cols] = dot(buf[...], w_in[:, cols]).astype(bf16)
        return carry

    def mlp_copies(which):
        rows = rows_at(which)
        return (pltpu.make_async_copy(hobuf.at[:, 0:ff], ho_o.at[rows, 0:ff], osem.at[0]),
                pltpu.make_async_copy(acts.at[rows, 0:2 * ff], grads_o.at[rows, 0:2 * ff], osem.at[1]))

    def dy_unit(which):
        load(1, which)
        rows = rows_at(which)
        do_all[rows, :] = dot(buf[...], wo[...], NT).astype(bf16)
        d_hidden = dot(buf[...], wd[...], NT)
        a, u = acts[rows, 0:ff].astype(f32), acts[rows, ff:2 * ff].astype(f32)
        sig = jax.nn.sigmoid(a)
        act = a * sig
        hobuf[:, 0:ff] = (act * u).astype(bf16)
        acts[rows, 0:ff] = (d_hidden * u * sig * (1.0 + a * (1.0 - sig))).astype(bf16)
        acts[rows, ff:2 * ff] = (d_hidden * act).astype(bf16)
        for copy in mlp_copies(which):
            copy.start()

    def attend(step, rows_per_step):
        start, width = step * rows_per_step, (step + 1) * rows_per_step
        rows = pl.ds(start, rows_per_step)
        q, d_out = acts[rows, q_at], do_all[rows, :]
        k, v = acts[0:width, k_at], acts[0:width, v_at]
        scores = dot(q, k, NT) * scale
        square = (rows_per_step, rows_per_step)
        causal = lax.broadcasted_iota(jnp.int32, square, 0) >= lax.broadcasted_iota(jnp.int32, square, 1)
        last = jnp.where(causal, scores[:, start:width], -jnp.inf)
        scores = jnp.concatenate([scores[:, :start], last], axis=1) if step else last
        prob = jnp.exp(scores - jnp.max(scores, axis=1, keepdims=True))
        prob = prob * (1.0 / jnp.sum(prob, axis=1, keepdims=True))
        prob_low = prob.astype(bf16)
        out = dot(prob_low, v).astype(bf16)
        hobuf[pl.ds(start % chunk, rows_per_step), ff:ff + head_dim] = out
        delta = jnp.sum(d_out.astype(f32) * out.astype(f32), axis=1, keepdims=True)
        d_scores = (prob * (dot(d_out, v, NT) - delta)).astype(bf16)
        d_q = (dot(d_scores, k) * scale).astype(bf16)
        if width == seq_len:
            dk_acc[...] = dot(d_scores, q, TN)
            dv_acc[...] = dot(prob_low, d_out, TN)
        else:
            dk_acc[0:width, :] += dot(d_scores, q, TN)
            dv_acc[0:width, :] += dot(prob_low, d_out, TN)
        acts[rows, q_at] = d_q
        acts[rows, k_at] = (dk_acc[rows, :] * scale).astype(bf16)
        acts[rows, v_at] = dv_acc[rows, :].astype(bf16)

    def attention_copies(which):
        rows = rows_at(which)
        return (pltpu.make_async_copy(hobuf.at[:, ff:ff + head_dim], ho_o.at[rows, ff:ff + head_dim], osem.at[2]),
                pltpu.make_async_copy(acts.at[rows, 2 * ff:width_in], grads_o.at[rows, 2 * ff:width_in], osem.at[3]))

    def dx_copy(which):
        return pltpu.make_async_copy(dxbuf, dx_o.at[rows_at(which)], osem.at[4])

    lax.fori_loop(0, CHIPS, x_unit, 0)

    def dy_step(step, carry):
        @pl.when((step > 0) & (step < CHIPS))
        def _():
            event(2 * step + 4)
            event(2 * step + 5)

        @pl.when(step < CHIPS)
        def _():
            dy_unit(look_up(DY_ORDER, step))

        @pl.when(step > 0)
        def _():
            which = CHIPS - step
            for static in range(CHIPS):
                @pl.when(which == static)
                def _():
                    for part in (1, 0):
                        attend(2 * static + part, piece)

            for copy in attention_copies(which):
                copy.start()

            @pl.when(step > 1)
            def _():
                dx_copy(which + 1).wait()
            for cut in range(2):
                cols = slice(cut * d_model // 2, (cut + 1) * d_model // 2)
                dxbuf[:, cols] = dot(acts[rows_at(which), :], w_in[cols, :], NT).astype(bf16)
            dx_copy(which).start()
            for copy in attention_copies(which):
                copy.wait()

        @pl.when(step < CHIPS)
        def _():
            for copy in mlp_copies(look_up(DY_ORDER, step)):
                copy.wait()
        return carry

    lax.fori_loop(0, CHIPS + 1, dy_step, 0)
    dx_copy(0).wait()

    def drain(i, carry):
        for array in range(2):
            for part in range(2):
                block = 2 * i + core
                remote(array, block, part, 2).wait_send()

                @pl.when((i <= chip) & (chip < CHIPS - 1))
                def _():
                    remote(array, block, part, 0).wait_send()

                @pl.when((i >= chip) & (chip > 0))
                def _():
                    remote(array, block, part, 1).wait_send()
        return carry
    lax.fori_loop(0, CHIPS, drain, 0)


def layer(x_loc, dy_loc, w_gate, w_up, w_q, w_k, w_v, w_down, w_o):
    piece, d_model = x_loc.shape
    seq_len, chunk = 2 * CHIPS * piece, 2 * piece
    ff, head_dim = w_down.shape[0], w_o.shape[0]
    width_in = 2 * ff + 3 * head_dim
    anywhere = pl.BlockSpec(memory_space=pl.ANY)
    shape = lambda *dims: jax.ShapeDtypeStruct(dims, bf16)
    vmem = lambda *dims: pltpu.VMEM(dims, bf16)
    dma = pltpu.SemaphoreType.DMA
    return pl.pallas_call(
        layer_kernel,
        out_shape=[shape(2 * seq_len, d_model), shape(seq_len, ff + head_dim), shape(seq_len, width_in)]
        + [shape(seq_len, d_model)],
        in_specs=[anywhere] * 9,
        out_specs=[anywhere] * 4,
        scratch_shapes=[vmem(d_model, width_in), vmem(ff, d_model), vmem(head_dim, d_model), vmem(chunk, d_model),
                        vmem(seq_len, width_in), vmem(seq_len, head_dim)]
        + [pltpu.VMEM((seq_len, head_dim), f32)] * 2
        + [vmem(chunk, ff + head_dim), vmem(chunk, d_model),
           dma((2, 2 * CHIPS, 2)), dma((3, 2, CHIPS, 2)), dma((7,)), dma((2,)), dma((5,))],
        compiler_params=pltpu.CompilerParams(vmem_limit_bytes=67043328, collective_id=0, has_side_effects=True),
        cost_estimate=pl.CostEstimate(flops=90 * 10 ** 9, bytes_accessed=80 * 2 ** 20, transcendentals=10 ** 7),
        name="layer")(x_loc, dy_loc, w_gate, w_up, w_q, w_k, w_v, w_down, w_o)


def input_grads_kernel(x_ref, g_ref, *outs):
    x = x_ref[...]
    start = 0
    for out in outs:
        width = out.shape[-1]
        product = dot(x, g_ref[:, start:start + width], TN)
        out[...] = product[:, None, :] if len(out.shape) == 3 else product
        start += width


def input_grads(xy, grads, ff, head_dim, tile=256):
    depth, width = grads.shape
    d_model = xy.shape[1]
    widths = (ff, ff, head_dim, head_dim, head_dim)
    return pl.pallas_call(
        input_grads_kernel,
        grid=(d_model // tile,),
        out_shape=[jax.ShapeDtypeStruct((d_model, 1, w) if i == 2 else (d_model, w), f32) for i, w in enumerate(widths)],
        in_specs=[pl.BlockSpec((depth, tile), lambda i: (0, i)),
                  pl.BlockSpec((depth, width), lambda i: (0, 0), pipeline_mode=pl.Buffered(1))],
        out_specs=[pl.BlockSpec((tile, 1, w), lambda i: (i, 0, 0)) if j == 2 else pl.BlockSpec((tile, w), lambda i: (i, 0))
                   for j, w in enumerate(widths)],
        compiler_params=pltpu.CompilerParams(vmem_limit_bytes=60 * 2 ** 20),
        cost_estimate=pl.CostEstimate(flops=2 * depth * width * d_model, bytes_accessed=2 * depth * (width + d_model)
                                      + 4 * width * d_model, transcendentals=0),
        name="input_grads")(xy, grads)


def output_grads_kernel(ho_ref, dy_ref, down_ref, o_ref):
    ff = down_ref.shape[0]
    down_ref[...] = dot(ho_ref[:, 0:ff], dy_ref[...], TN)
    o_ref[0] = dot(ho_ref[:, ff:], dy_ref[...], TN)


def output_grads(ho, xy, ff, head_dim, tile=384):
    depth, width = ho.shape
    d_model = xy.shape[1]
    return pl.pallas_call(
        output_grads_kernel,
        grid=(d_model // tile,),
        out_shape=[jax.ShapeDtypeStruct((ff, d_model), f32), jax.ShapeDtypeStruct((1, head_dim, d_model), f32)],
        in_specs=[pl.BlockSpec((depth, width), lambda i: (0, 0), pipeline_mode=pl.Buffered(1)),
                  pl.BlockSpec((depth, tile), lambda i: (1, i))],
        out_specs=[pl.BlockSpec((ff, tile), lambda i: (0, i)), pl.BlockSpec((1, head_dim, tile), lambda i: (0, 0, i))],
        compiler_params=pltpu.CompilerParams(vmem_limit_bytes=60 * 2 ** 20),
        cost_estimate=pl.CostEstimate(flops=2 * depth * width * d_model, bytes_accessed=2 * depth * (width + d_model)
                                      + 4 * width * d_model, transcendentals=0),
        name="output_grads")(ho, xy)


def solution(mesh):
    tp_count = mesh.shape["tp"]

    def swap(value):
        return lax.ppermute(value, "tp", [(i, i ^ 1) for i in range(tp_count)])

    def local_step(x_loc, dy_loc, w_q, w_k, w_v, w_o, w_gate, w_up, w_down):
        rank = lax.axis_index("tp")
        core = rank % 2
        kv_index = rank // 2
        wk_one = lax.dynamic_index_in_dim(w_k, kv_index, axis=1, keepdims=False)
        wv_one = lax.dynamic_index_in_dim(w_v, kv_index, axis=1, keepdims=False)
        ff, head_dim = w_down.shape[0], w_o.shape[1]
        xy, ho, grads, dx_all = layer(
            x_loc, dy_loc, w_gate, w_up, w_q[:, 0, :], wk_one, wv_one, w_down, w_o[0])
        dx_loc = lax.psum_scatter(dx_all, "tp", scatter_dimension=0, tiled=True)
        dw_gate, dw_up, dw_q, dwk_part, dwv_part = input_grads(xy, grads, ff, head_dim)
        stacked = jnp.stack([dwk_part, dwv_part])
        half = stacked.shape[1] // 2
        keep = lax.dynamic_slice_in_dim(stacked, core * half, half, axis=1)
        send = lax.dynamic_slice_in_dim(stacked, (1 - core) * half, half, axis=1)
        kv_grads = keep + swap(send)
        dw_down, dw_o = output_grads(ho, xy, ff, head_dim)
        return (dx_loc, dw_q, kv_grads[0:1], kv_grads[1:2], dw_o, dw_gate, dw_up, dw_down)

    token_spec = P(("dp", "tp"), None)
    in_specs = (token_spec, token_spec, P(None, "tp", None), P(None, None, None), P(None, None, None),
                P("tp", None, None), P(None, "tp"), P(None, "tp"), P("tp", None))
    out_specs = (token_spec, P("dp", "tp", None), P(("dp", "tp"), None, None), P(("dp", "tp"), None, None),
                 P(("dp", "tp"), None, None), P("dp", "tp"), P("dp", "tp"), P(("dp", "tp"), None))
    return jax.shard_map(local_step, mesh=mesh, in_specs=in_specs, out_specs=out_specs, check_vma=False)
```

```python
import functools
import jax
import jax.numpy as jnp
from jax import lax
from jax.experimental import pallas as pl
from jax.experimental.pallas import tpu as pltpu
from jax.sharding import PartitionSpec as P


f32, bf16 = jnp.float32, jnp.bfloat16
NT = (((1,), (1,)), ((), ()))
TN = (((0,), (0,)), ((), ()))
NN = (((1,), (0,)), ((), ()))


def dot(a, b, dims=NN):
    return lax.dot_general(a, b, dims, preferred_element_type=f32)


def pick(chip, values):
    out = jnp.int32(values[-1])
    for i in range(len(values) - 1):
        out = jnp.where(chip == i, jnp.int32(values[i]), out)
    return out


X_ORDER = ((0, 1, 2, 3), (1, 0, 2, 3), (2, 3, 1, 0), (3, 2, 1, 0))
DY_ORDER = ((0, 3, 2, 1), (1, 3, 2, 0), (2, 3, 1, 0), (3, 2, 1, 0))
CHIPS = 4


def layer_kernel(x_loc, dy_loc, wg_h, wu_h, wq_h, wk_h, wv_h, wd_h, wo_h,
                 xy, ho_o, grads_o, dx_o,
                 w_in, wd, wo, buf, acts, do_all, dk_acc, dv_acc,
                 hobuf, dxbuf, early, recv, send, wsem, lsem, osem):
    piece, d_model = x_loc.shape
    seq_len = CHIPS * 2 * piece
    chunk = 2 * piece
    half = piece // 2
    head_dim = wo.shape[0]
    ff = wd.shape[0]
    width_in = acts.shape[1]
    q_at, k_at, v_at = (slice(2 * ff + i * head_dim, 2 * ff + (i + 1) * head_dim) for i in range(3))
    scale = head_dim ** -0.5
    me = lax.axis_index("tp")
    chip, core = me // 2, me % 2
    partner = me + 1 - 2 * core
    own = (x_loc, dy_loc)

    barrier = pltpu.get_barrier_semaphore()
    for step in range(1, 2 * CHIPS):
        pl.semaphore_signal(barrier, inc=1, device_id={"tp": (me + step) % (2 * CHIPS)},
                            device_id_type=pl.DeviceIdType.MESH)
    weights = [pltpu.make_async_copy(src, dst, wsem.at[i]) for i, (src, dst) in enumerate(
        ((wg_h, w_in.at[:, 0:ff]), (wu_h, w_in.at[:, ff:2 * ff]), (wq_h, w_in.at[:, q_at]), (wk_h, w_in.at[:, k_at]),
         (wv_h, w_in.at[:, v_at]), (wd_h, wd), (wo_h, wo)))]
    for copy in weights:
        copy.start()
    pl.semaphore_wait(barrier, 2 * CHIPS - 1)

    def rows_of(array, block, part):
        return pl.ds(pl.multiple_of(array * seq_len + block * piece + part * half, half), half)

    def remote(array, block, part, way, own_source=None):
        target = (me + 2, me - 2, partner)[way]
        there = xy.at[rows_of(array, block, part)]
        source = there if own_source is None else own_source.at[pl.ds(part * half, half)]
        return pltpu.make_async_remote_copy(
            src_ref=source, dst_ref=there, send_sem=send.at[way, array, block // 2, part],
            recv_sem=recv.at[array, block, part], device_id={"tp": target}, device_id_type=pl.DeviceIdType.MESH)

    def send_own(array, way):
        for part in range(2):
            remote(array, me, part, way, own[array]).start()

    @pl.when(chip < CHIPS - 1)
    def _():
        send_own(0, 0)

    @pl.when(chip > 0)
    def _():
        send_own(0, 1)

    send_own(0, 2)
    send_own(1, 2)

    def event(k):
        j, part = k // 2, k % 2

        @pl.when((chip < CHIPS - 1) & (2 * chip == k))
        def _():
            send_own(1, 0)

        @pl.when((chip > 0) & (4 * (CHIPS - 1 - chip) == k))
        def _():
            send_own(1, 1)

        above = CHIPS - 1 - chip

        @pl.when(j < 2 * above)
        def _():
            array = jnp.where(j < above, 0, 1)
            block = 2 * jnp.where(j < above, chip + 1 + j, CHIPS - 1 - j + above) + core
            remote(array, block, part, 2).wait_recv()
            remote(array, block, part, 2).start()

            @pl.when(chip > 0)
            def _():
                remote(array, block, part, 1).start()

        below = chip

        @pl.when(j < 2 * below)
        def _():
            array = jnp.where(j < below, 0, 1)
            block = 2 * jnp.where(j < below, chip - 1 - j, chip - 1 - j + below) + core
            remote(array, block, part, 2).wait_recv()
            remote(array, block, part, 2).start()

            @pl.when(chip < CHIPS - 1)
            def _():
                remote(array, block, part, 0).start()

    def load(array, which):
        for part in range(2):
            remote(array, 2 * which + 1 - core, part, 2).wait_recv()
        copy = pltpu.make_async_copy(xy.at[pl.ds(pl.multiple_of(array * seq_len + which * chunk, chunk), chunk)],
                                     buf, lsem.at[0])
        copy.start()
        copy.wait()

    def rows_at(which):
        return pl.ds(pl.multiple_of(which * chunk, chunk), chunk)

    def look_up(orders, unit):
        return pick(unit, [pick(chip, [order[i] for order in orders]) for i in range(CHIPS)])

    keeps = [pltpu.make_async_copy(src, dxbuf.at[pl.ds(i * piece, piece)], lsem.at[i]) for i, src in enumerate(own)]
    for copy in keeps:
        copy.start()
    for copy in keeps:
        copy.wait()
    keeps = [pltpu.make_async_copy(dxbuf.at[pl.ds(i * piece, piece)],
                                   xy.at[pl.ds(pl.multiple_of(i * seq_len + me * piece, piece), piece)], lsem.at[i])
             for i in range(2)]
    for copy in keeps:
        copy.start()
    for copy in keeps:
        copy.wait()
    for copy in weights:
        copy.wait()

    def x_unit(unit, carry):
        @pl.when(unit > 0)
        def _():
            event(2 * unit - 2)
            event(2 * unit - 1)

        which = look_up(X_ORDER, unit)
        load(0, which)
        for cut in range(2):
            cols = slice(cut * width_in // 2, (cut + 1) * width_in // 2)
            acts[rows_at(which), cols] = dot(buf[...], w_in[:, cols]).astype(bf16)
        return carry

    def mlp_copies(which):
        rows = rows_at(which)
        return (pltpu.make_async_copy(hobuf.at[:, 0:ff], ho_o.at[rows, 0:ff], osem.at[0]),
                pltpu.make_async_copy(acts.at[rows, 0:2 * ff], grads_o.at[rows, 0:2 * ff], osem.at[1]))

    def dy_unit(which):
        load(1, which)
        rows = rows_at(which)
        do_all[rows, :] = dot(buf[...], wo[...], NT).astype(bf16)
        d_hidden = dot(buf[...], wd[...], NT)
        a, u = acts[rows, 0:ff].astype(f32), acts[rows, ff:2 * ff].astype(f32)
        sig = jax.nn.sigmoid(a)
        act = a * sig
        hobuf[:, 0:ff] = (act * u).astype(bf16)
        acts[rows, 0:ff] = (d_hidden * u * sig * (1.0 + a * (1.0 - sig))).astype(bf16)
        acts[rows, ff:2 * ff] = (d_hidden * act).astype(bf16)
        for copy in mlp_copies(which):
            copy.start()

    def attend(step, rows_per_step):
        start, width = step * rows_per_step, (step + 1) * rows_per_step
        rows = pl.ds(start, rows_per_step)
        q, d_out = acts[rows, q_at], do_all[rows, :]
        k, v = acts[0:width, k_at], acts[0:width, v_at]
        scores = dot(q, k, NT) * scale
        square = (rows_per_step, rows_per_step)
        causal = lax.broadcasted_iota(jnp.int32, square, 0) >= lax.broadcasted_iota(jnp.int32, square, 1)
        last = jnp.where(causal, scores[:, start:width], -jnp.inf)
        scores = jnp.concatenate([scores[:, :start], last], axis=1) if step else last
        prob = jnp.exp(scores - jnp.max(scores, axis=1, keepdims=True))
        prob = prob * (1.0 / jnp.sum(prob, axis=1, keepdims=True))
        prob_low = prob.astype(bf16)
        out = dot(prob_low, v).astype(bf16)
        hobuf[pl.ds(start % chunk, rows_per_step), ff:ff + head_dim] = out
        delta = jnp.sum(d_out.astype(f32) * out.astype(f32), axis=1, keepdims=True)
        d_scores = (prob * (dot(d_out, v, NT) - delta)).astype(bf16)
        d_q = (dot(d_scores, k) * scale).astype(bf16)
        if width == seq_len:
            dk_acc[...] = dot(d_scores, q, TN)
            dv_acc[...] = dot(prob_low, d_out, TN)
        else:
            dk_acc[0:width, :] += dot(d_scores, q, TN)
            dv_acc[0:width, :] += dot(prob_low, d_out, TN)
        acts[rows, q_at] = d_q
        acts[rows, k_at] = (dk_acc[rows, :] * scale).astype(bf16)
        acts[rows, v_at] = dv_acc[rows, :].astype(bf16)

    def attention_copies(which):
        rows = rows_at(which)
        return (pltpu.make_async_copy(hobuf.at[:, ff:ff + head_dim], ho_o.at[rows, ff:ff + head_dim], osem.at[2]),
                pltpu.make_async_copy(acts.at[rows, 2 * ff:width_in], grads_o.at[rows, 2 * ff:width_in], osem.at[3]))

    def dx_copy(which):
        return pltpu.make_async_copy(dxbuf, dx_o.at[rows_at(which)], osem.at[4])

    lax.fori_loop(0, CHIPS, x_unit, 0)

    def dy_step(step, carry):
        @pl.when((step > 0) & (step < CHIPS))
        def _():
            event(2 * step + 4)
            event(2 * step + 5)

        @pl.when(step < CHIPS)
        def _():
            dy_unit(look_up(DY_ORDER, step))

        @pl.when((step == 0) & (chip == 0))
        def _():
            for cut in range(2):
                cols = slice(cut * d_model // 2, (cut + 1) * d_model // 2)
                early[:, cols] = dot(acts[0:chunk, 0:2 * ff], w_in[cols, 0:2 * ff], NT)

        which = jnp.where(chip == CHIPS - 1, CHIPS - 1, CHIPS) - step

        @pl.when((which >= 0) & (which < CHIPS))
        def _():
            for static in range(CHIPS):
                @pl.when(which == static)
                def _():
                    for part in (1, 0):
                        attend(2 * static + part, piece)

            for copy in attention_copies(which):
                copy.start()

            @pl.when(which < CHIPS - 1)
            def _():
                dx_copy(which + 1).wait()

            @pl.when((which == 0) & (chip == 0))
            def _():
                late = dot(acts[0:chunk, 2 * ff:width_in], w_in[:, 2 * ff:width_in], NT)
                dxbuf[...] = (early[...] + late).astype(bf16)

            @pl.when((which > 0) | (chip > 0))
            def _():
                for cut in range(2):
                    cols = slice(cut * d_model // 2, (cut + 1) * d_model // 2)
                    dxbuf[:, cols] = dot(acts[rows_at(which), :], w_in[cols, :], NT).astype(bf16)
            dx_copy(which).start()
            for copy in attention_copies(which):
                copy.wait()

        @pl.when(step < CHIPS)
        def _():
            for copy in mlp_copies(look_up(DY_ORDER, step)):
                copy.wait()
        return carry

    lax.fori_loop(0, CHIPS + 1, dy_step, 0)
    dx_copy(0).wait()

    def drain(i, carry):
        for array in range(2):
            for part in range(2):
                block = 2 * i + core
                remote(array, block, part, 2).wait_send()

                @pl.when((i <= chip) & (chip < CHIPS - 1))
                def _():
                    remote(array, block, part, 0).wait_send()

                @pl.when((i >= chip) & (chip > 0))
                def _():
                    remote(array, block, part, 1).wait_send()
        return carry
    lax.fori_loop(0, CHIPS, drain, 0)


def layer(x_loc, dy_loc, w_gate, w_up, w_q, w_k, w_v, w_down, w_o):
    piece, d_model = x_loc.shape
    seq_len, chunk = 2 * CHIPS * piece, 2 * piece
    ff, head_dim = w_down.shape[0], w_o.shape[0]
    width_in = 2 * ff + 3 * head_dim
    anywhere = pl.BlockSpec(memory_space=pl.ANY)
    shape = lambda *dims: jax.ShapeDtypeStruct(dims, bf16)
    vmem = lambda *dims: pltpu.VMEM(dims, bf16)
    dma = pltpu.SemaphoreType.DMA
    return pl.pallas_call(
        layer_kernel,
        out_shape=[shape(2 * seq_len, d_model), shape(seq_len, ff + head_dim), shape(seq_len, width_in)]
        + [shape(seq_len, d_model)],
        in_specs=[anywhere] * 9,
        out_specs=[anywhere] * 4,
        scratch_shapes=[vmem(d_model, width_in), vmem(ff, d_model), vmem(head_dim, d_model), vmem(chunk, d_model),
                        vmem(seq_len, width_in), vmem(seq_len, head_dim)]
        + [pltpu.VMEM((seq_len, head_dim), f32)] * 2
        + [vmem(chunk, ff + head_dim), vmem(chunk, d_model), pltpu.VMEM((chunk, d_model), f32),
           dma((2, 2 * CHIPS, 2)), dma((3, 2, CHIPS, 2)), dma((7,)), dma((2,)), dma((5,))],
        compiler_params=pltpu.CompilerParams(vmem_limit_bytes=67043328, collective_id=0, has_side_effects=True),
        cost_estimate=pl.CostEstimate(flops=90 * 10 ** 9, bytes_accessed=80 * 2 ** 20, transcendentals=10 ** 7),
        name="layer")(x_loc, dy_loc, w_gate, w_up, w_q, w_k, w_v, w_down, w_o)


def input_grads_kernel(x_ref, g_ref, *outs):
    x = x_ref[...]
    start = 0
    for out in outs:
        width = out.shape[-1]
        product = dot(x, g_ref[:, start:start + width], TN)
        out[...] = product[:, None, :] if len(out.shape) == 3 else product
        start += width


def input_grads(xy, grads, ff, head_dim, tile=256):
    depth, width = grads.shape
    d_model = xy.shape[1]
    widths = (ff, ff, head_dim, head_dim, head_dim)
    return pl.pallas_call(
        input_grads_kernel,
        grid=(d_model // tile,),
        out_shape=[jax.ShapeDtypeStruct((d_model, 1, w) if i == 2 else (d_model, w), f32) for i, w in enumerate(widths)],
        in_specs=[pl.BlockSpec((depth, tile), lambda i: (0, i)),
                  pl.BlockSpec((depth, width), lambda i: (0, 0), pipeline_mode=pl.Buffered(1))],
        out_specs=[pl.BlockSpec((tile, 1, w), lambda i: (i, 0, 0)) if j == 2 else pl.BlockSpec((tile, w), lambda i: (i, 0))
                   for j, w in enumerate(widths)],
        compiler_params=pltpu.CompilerParams(vmem_limit_bytes=60 * 2 ** 20),
        cost_estimate=pl.CostEstimate(flops=2 * depth * width * d_model, bytes_accessed=2 * depth * (width + d_model)
                                      + 4 * width * d_model, transcendentals=0),
        name="input_grads")(xy, grads)


def output_grads_kernel(ho_ref, dy_ref, down_ref, o_ref):
    ff = down_ref.shape[0]
    down_ref[...] = dot(ho_ref[:, 0:ff], dy_ref[...], TN)
    o_ref[0] = dot(ho_ref[:, ff:], dy_ref[...], TN)


def output_grads(ho, xy, ff, head_dim, tile=384):
    depth, width = ho.shape
    d_model = xy.shape[1]
    return pl.pallas_call(
        output_grads_kernel,
        grid=(d_model // tile,),
        out_shape=[jax.ShapeDtypeStruct((ff, d_model), f32), jax.ShapeDtypeStruct((1, head_dim, d_model), f32)],
        in_specs=[pl.BlockSpec((depth, width), lambda i: (0, 0), pipeline_mode=pl.Buffered(1)),
                  pl.BlockSpec((depth, tile), lambda i: (1, i))],
        out_specs=[pl.BlockSpec((ff, tile), lambda i: (0, i)), pl.BlockSpec((1, head_dim, tile), lambda i: (0, 0, i))],
        compiler_params=pltpu.CompilerParams(vmem_limit_bytes=60 * 2 ** 20),
        cost_estimate=pl.CostEstimate(flops=2 * depth * width * d_model, bytes_accessed=2 * depth * (width + d_model)
                                      + 4 * width * d_model, transcendentals=0),
        name="output_grads")(ho, xy)


def solution(mesh):
    tp_count = mesh.shape["tp"]

    def swap(value):
        return lax.ppermute(value, "tp", [(i, i ^ 1) for i in range(tp_count)])

    def local_step(x_loc, dy_loc, w_q, w_k, w_v, w_o, w_gate, w_up, w_down):
        rank = lax.axis_index("tp")
        core = rank % 2
        kv_index = rank // 2
        wk_one = lax.dynamic_index_in_dim(w_k, kv_index, axis=1, keepdims=False)
        wv_one = lax.dynamic_index_in_dim(w_v, kv_index, axis=1, keepdims=False)
        ff, head_dim = w_down.shape[0], w_o.shape[1]
        xy, ho, grads, dx_all = layer(
            x_loc, dy_loc, w_gate, w_up, w_q[:, 0, :], wk_one, wv_one, w_down, w_o[0])
        dx_loc = lax.psum_scatter(dx_all, "tp", scatter_dimension=0, tiled=True)
        dw_gate, dw_up, dw_q, dwk_part, dwv_part = input_grads(xy, grads, ff, head_dim)
        stacked = jnp.stack([dwk_part, dwv_part])
        half = stacked.shape[1] // 2
        keep = lax.dynamic_slice_in_dim(stacked, core * half, half, axis=1)
        send = lax.dynamic_slice_in_dim(stacked, (1 - core) * half, half, axis=1)
        kv_grads = keep + swap(send)
        dw_down, dw_o = output_grads(ho, xy, ff, head_dim)
        return (dx_loc, dw_q, kv_grads[0:1], kv_grads[1:2], dw_o, dw_gate, dw_up, dw_down)

    token_spec = P(("dp", "tp"), None)
    in_specs = (token_spec, token_spec, P(None, "tp", None), P(None, None, None), P(None, None, None),
                P("tp", None, None), P(None, "tp"), P(None, "tp"), P("tp", None))
    out_specs = (token_spec, P("dp", "tp", None), P(("dp", "tp"), None, None), P(("dp", "tp"), None, None),
                 P(("dp", "tp"), None, None), P("dp", "tp"), P("dp", "tp"), P(("dp", "tp"), None))
    return jax.shard_map(local_step, mesh=mesh, in_specs=in_specs, out_specs=out_specs, check_vma=False)
```
